32 devices in a mesh: dp: 8 (over z, x), mp: 4 (over y, core).
Axes of the slice: x: 2, y: 2, z: 4, core: 2. Of those that a mesh axis runs over, the one named last changes fastest.
Arguments:
- x_in: bfloat16 [32768, 768], P(('dp', 'mp')), may hold values from -6 to 6
- segments: int32 [32, 1024], P(('dp', 'mp')), may hold values from 0 to 4, never falling along the last dimension, each value on 1 to 312 neighbouring positions
- targets: bfloat16 [32768, 1024], P(('dp', 'mp')), may hold values from -6 to 6
- cotangent: bfloat16 [32768, 768], P(('dp', 'mp')), may hold values from -6 to 6
- norm_gain: float32 [3, 768], replicated, may hold values from 0.5 to 1.5
- norm_bias: float32 [3, 768], replicated, may hold values from -1.5 to 1.5
- attn_w: float32 [768, 4096], P(('dp', 'mp'))
- mlp_w: float32 [2, 768, 3072], P(None, 'dp', 'mp'), may hold values from -0.21875 to 0.21875
- norm_first: float32 [6, 768], replicated, may hold values from -128 to 128
- norm_second: float32 [6, 768], replicated, may hold values from 32.768 to 131.072
- attn_first: float32 [768, 4096], P(('dp', 'mp')), may hold values from -128 to 128
- attn_second: float32 [768, 4096], P(('dp', 'mp')), may hold values from 32.768 to 131.072
- mlp_first: float32 [2, 768, 3072], P(None, 'dp', 'mp'), may hold values from -128 to 128
- mlp_second: float32 [2, 768, 3072], P(None, 'dp', 'mp'), may hold values from 32.768 to 131.072
Outputs:
- y_out: bfloat16 [32768, 768], P(('dp', 'mp'))
- x_grad: float32 [32768, 768], P(('dp', 'mp'))
- attn_new: float32 [768, 4096], P(('dp', 'mp'))
- attn_first_new: float32 [768, 4096], P(('dp', 'mp'))
- attn_second_new: float32 [768, 4096], P(('dp', 'mp'))
- mlp_new: float32 [2, 768, 3072], P(None, 'dp', 'mp')
- mlp_first_new: float32 [2, 768, 3072], P(None, 'dp', 'mp')
- mlp_second_new: float32 [2, 768, 3072], P(None, 'dp', 'mp')
- norm_new: float32 [6, 768], replicated
- norm_first_new: float32 [6, 768], replicated
- norm_second_new: float32 [6, 768], replicated
- lamb_norms: float32 [2, 5], replicated
The draws below stay inside these ranges and needn't reach their ends.
Inputs may be any that keep to these rules, and one draw needn't show every extreme that they name: `segments`: each row is one device's tokens: a packed run of whole clips, ids never fall along the row, each clip has 1 to 312 tokens and one has exactly 312.
All inputs are finite; a program needn't handle non-finite values.
Results may differ from the reference program's by a relative error of at most 0.015.
Values may be sent and summed in bfloat16 or wider, within the bound.
A program may use at most 256 MiB of HBM per device.

```python
import math
import jax
import jax.numpy as jnp
import numpy as np
from jax import lax

D = 768
H = 12
HD = 64
FF = 3072
TD = 1024
TOK_DEV = 1024
STEP = 10
TOKENS = 32768
LONGEST = 312
SEGS = 5
COLS = 4096
DEVICES = 32


def draw_attn_w(key, part):
    values = jax.random.truncated_normal(key, -4.0, 4.0, (D, 4 * D + TD), jnp.float32)
    column = jnp.arange(4 * D + TD)
    boost = jnp.where((column >= 3 * D) & (column < 4 * D), 4.0, 1.0)
    return values * boost[None, :] * D ** (-0.5)


def shard_levels(own_key, extent, shards, low, top_value):
    factor_of, own = 1.0, jax.random.fold_in(own_key, 6)
    for position, parts in shards:
        draws = jnp.exp(jax.random.uniform(jax.random.fold_in(own, position), (parts,), jnp.float32, low / len(shards), top_value / len(shards)))
        factor_of = factor_of * jnp.repeat(draws, extent[position] // parts).reshape([-1 if axis == position else 1 for axis in range(len(extent))])
    return factor_of


def profile(number_of, total, limit, slope):
    portions = [(1 << 20) // math.isqrt(grade ** slope) + 1 for grade in range(2, number_of + 1)]
    surplus, counts = total - limit - (number_of - 1), [1] * (number_of - 1)
    while surplus > 0:
        movable = [i for i in range(number_of - 1) if counts[i] < limit]
        mass, left = sum([portions[i] for i in movable]), surplus
        for i in movable:
            addition = min(limit - counts[i], max(1, left * portions[i] // mass), surplus)
            counts[i] = counts[i] + addition
            surplus = surplus - addition
    return np.array([limit] + counts)


def ragged(own_key, number_of, total, limit, skew):
    if number_of == 2:
        one = jax.random.randint(own_key, (), max(1, total - limit), min(limit, total - 1) + 1)
        return jnp.stack([one, total - one])
    sizes = jnp.asarray(profile(number_of, total, limit, skew), jnp.int32)
    couples = (number_of - 1) // 2
    source_of, receiver = sizes[1:1 + 2 * couples:2], sizes[2:2 + 2 * couples:2]
    room = jnp.minimum(source_of - 1, limit - receiver)
    shifted = jax.random.randint(jax.random.fold_in(own_key, 1), (couples,), 0, 1 << 20) % (room + 1)
    sizes = sizes.at[1:1 + 2 * couples:2].set(source_of - shifted).at[2:2 + 2 * couples:2].set(receiver + shifted)
    return sizes[jax.random.permutation(jax.random.fold_in(own_key, 2), number_of)]


def bell_draw(key, extent, spread, reach, cuts=(), held_as=jnp.bfloat16):
    array = spread * jax.random.normal(key, extent, jnp.float32)
    if cuts:
        array = array * shard_levels(key, extent, cuts, -0.22, 0.18)
    return jnp.clip(array, -reach, reach).astype(held_as)


def setup_inputs(seed: int = 0) -> dict:
    key_of = jax.random.split(jax.random.key(seed), 15)
    return {
        "x_in": bell_draw(key_of[0], (TOKENS, D), 1.0, 6.0, ((0, 32),)),
        "segments": jax.vmap(lambda own: jnp.searchsorted(jnp.cumsum(ragged(own, SEGS, TOK_DEV, LONGEST, 2)), jnp.arange(TOK_DEV), side="right"))(jax.random.split(key_of[1], DEVICES)).reshape((DEVICES, TOK_DEV)).astype(jnp.int32),
        "targets": bell_draw(key_of[2], (TOKENS, TD), 1.0, 6.0, ((0, 32),)),
        "cotangent": bell_draw(key_of[3], (TOKENS, D), 1.0, 6.0, ((0, 32),)),
        "norm_gain": jnp.clip(1.0 + 0.1 * jax.random.normal(key_of[4], (3, D), jnp.float32), 0.5, 1.5),
        "norm_bias": bell_draw(key_of[5], (3, D), 0.3, 1.5, (), jnp.float32),
        "attn_w": draw_attn_w(jax.random.fold_in(key_of[14], 71), 0),
        "mlp_w": bell_draw(key_of[7], (2, D, FF), D ** -0.5, 0.21875, ((1, 8), (2, 4)), jnp.float32),
        "norm_first": bell_draw(key_of[8], (6, D), (0.11 * TOKENS ** 0.5), 128.0, (), jnp.float32),
        "norm_second": jnp.clip(jnp.exp(jax.random.uniform(key_of[9], (6, D), jnp.float32, math.log(32.768), math.log(131.072))), 32.768, 131.072),
        "attn_first": bell_draw(key_of[10], (D, COLS), (0.11 * TOKENS ** 0.5), 128.0, ((0, 32),), jnp.float32),
        "attn_second": jnp.clip(jnp.exp(math.log(131.072) - 1.3862944 * jax.random.uniform(key_of[11], (D, COLS), jnp.float32) ** shard_levels(key_of[11], (D, COLS), ((0, 32),), -0.2, 0.2)), 32.768, 131.072),
        "mlp_first": bell_draw(key_of[12], (2, D, FF), (0.11 * TOKENS ** 0.5), 128.0, ((1, 8), (2, 4)), jnp.float32),
        "mlp_second": jnp.clip(jnp.exp(math.log(131.072) - 1.3862944 * jax.random.uniform(key_of[13], (2, D, FF), jnp.float32) ** shard_levels(key_of[13], (2, D, FF), ((1, 8), (2, 4)), -0.2, 0.2)), 32.768, 131.072),
    }


@jax.custom_vjp
def low(v):
    return lax.optimization_barrier(v.astype(jnp.bfloat16)).astype(jnp.float32)

@jax.custom_vjp
def low_back(v):
    return v

def low_keep(v):
    return (low(v), None)

def low_pass(kept, grad):
    return (grad,)

def back_keep(v):
    return (v, None)

def back_low(kept, grad):
    return (low(grad),)
low.defvjp(low_keep, low_pass)
low_back.defvjp(back_keep, back_low)
HIGH = lax.Precision.HIGHEST
eps_norm = 1e-06
beta_one = 0.9
beta_two = 0.999
eps_adam = 1e-06
decay_rate = 0.05
learn_rate = 0.3

def round_both(v):
    return low_back(low(v))

def layer_norm(values, gain_row, shift_row):
    centre = values - lax.optimization_barrier(jnp.mean(values, axis=-1, keepdims=True))
    inv_std = lax.rsqrt(lax.optimization_barrier(jnp.mean(centre * centre, axis=-1, keepdims=True)) + eps_norm)
    return centre * inv_std * gain_row + shift_row

def attend_rows(pair_rows):
    proj_rows, seg_row = pair_rows
    tok_count = proj_rows.shape[0]
    queries = proj_rows[:, :D].reshape(tok_count, H, HD)
    key_part = proj_rows[:, D:2 * D].reshape(tok_count, H, HD)
    value_part = proj_rows[:, 2 * D:].reshape(tok_count, H, HD)
    scores = jnp.einsum('qhd,khd->hqk', queries, key_part, precision=HIGH) * HD ** (-0.5)
    scores = low_back(scores)
    allowed = seg_row[:, None] == seg_row[None, :]
    scores = jnp.where(allowed[None], scores, -1e+30)
    row_max = lax.optimization_barrier(jnp.max(scores, axis=-1, keepdims=True))
    exp_scores = jnp.exp(scores - row_max)
    attn_prob = low(exp_scores / lax.optimization_barrier(jnp.sum(exp_scores, axis=-1, keepdims=True)))
    context = jnp.einsum('hqk,khd->qhd', attn_prob, value_part, precision=HIGH)
    return context.reshape(tok_count, D)

def forward(residual, norm_gain, norm_bias, attn_w, mlp_w, teacher, cot_grad, segments):
    w_attn = low(attn_w)
    w_mlp = low(mlp_w)
    w_qkv = w_attn[:, :3 * D]
    w_out = w_attn[:, 3 * D:4 * D]
    w_head = w_attn[:, 4 * D:]
    h_one = low(layer_norm(residual, norm_gain[0], norm_bias[0]))
    proj = round_both(jnp.dot(h_one, w_qkv, precision=HIGH))
    context = lax.map(jax.checkpoint(attend_rows), (proj.reshape(-1, TOK_DEV, 3 * D), segments))
    context = round_both(context.reshape(-1, D))
    middle = residual + low_back(jnp.dot(context, w_out, precision=HIGH))
    h_two = low(layer_norm(middle, norm_gain[1], norm_bias[1]))
    pre_act = low_back(jnp.dot(h_two, w_mlp[0], precision=HIGH))
    hidden = low(jax.nn.gelu(pre_act, approximate=False))
    block_out = middle + low_back(jnp.dot(hidden, w_mlp[1].T, precision=HIGH))
    h_three = low(layer_norm(block_out, norm_gain[2], norm_bias[2]))
    aligned = low_back(jnp.dot(h_three, w_head, precision=HIGH))
    inv_al = lax.rsqrt(lax.optimization_barrier(jnp.mean(aligned * aligned, axis=-1)) + eps_norm)
    inv_te = lax.rsqrt(lax.optimization_barrier(jnp.mean(teacher * teacher, axis=-1)) + eps_norm)
    cosine = lax.optimization_barrier(jnp.mean(aligned * teacher, axis=-1)) * inv_al * inv_te
    objective = jnp.sum(block_out * cot_grad) + TD * jnp.sum(1.0 - cosine)
    return (objective, block_out)

def moments(weight, gradient, first_old, second_old, wd_rate):
    first_new = beta_one * first_old + (1.0 - beta_one) * gradient
    second_new = beta_two * second_old + (1.0 - beta_two) * gradient * gradient
    corr_one = 1.0 - beta_one ** STEP
    corr_two = 1.0 - beta_two ** STEP
    update = first_new / corr_one / (jnp.sqrt(second_new / corr_two) + eps_adam) + wd_rate * weight
    return (first_new, second_new, update)

def reference(x_in, segments, targets, cotangent, norm_gain, norm_bias, attn_w, mlp_w, norm_first, norm_second, attn_first, attn_second, mlp_first, mlp_second):
    residual = x_in.astype(jnp.float32)
    teacher = targets.astype(jnp.float32)
    cot_grad = cotangent.astype(jnp.float32)

    def objective_fn(res_arg, gain_arg, bias_arg, attn_arg, mlp_arg):
        return forward(res_arg, gain_arg, bias_arg, attn_arg, mlp_arg, teacher, cot_grad, segments)
    value_total, pullback, block_out = jax.vjp(objective_fn, residual, norm_gain, norm_bias, attn_w, mlp_w, has_aux=True)
    grad_x, grad_gain, grad_bias, grad_attn, grad_mlp = pullback(jnp.ones_like(value_total))
    attn_first_new, attn_second_new, attn_update = moments(attn_w, grad_attn, attn_first, attn_second, decay_rate)
    mlp_first_new, mlp_second_new, mlp_update = moments(mlp_w, grad_mlp, mlp_first, mlp_second, decay_rate)
    norm_w = jnp.concatenate([norm_gain, norm_bias], axis=0)
    norm_g = jnp.concatenate([grad_gain, grad_bias], axis=0)
    norm_first_new, norm_second_new, norm_update = moments(norm_w, norm_g, norm_first, norm_second, 0.0)
    bounds = ((0, 3 * D), (3 * D, 4 * D), (4 * D, 4 * D + TD))
    weight_sq = [jnp.sum(attn_w[:, left_col:right_col] * attn_w[:, left_col:right_col]) for left_col, right_col in bounds]
    update_sq = [jnp.sum(attn_update[:, left_col:right_col] * attn_update[:, left_col:right_col]) for left_col, right_col in bounds]
    weight_sq = weight_sq + [jnp.sum(mlp_w[0] * mlp_w[0]), jnp.sum(mlp_w[1] * mlp_w[1])]
    update_sq = update_sq + [jnp.sum(mlp_update[0] * mlp_update[0]), jnp.sum(mlp_update[1] * mlp_update[1])]
    lamb_norms = jnp.sqrt(jnp.stack([jnp.stack(weight_sq), jnp.stack(update_sq)]))
    ratio = lamb_norms[0] / lamb_norms[1]
    ratio_cols = jnp.concatenate([jnp.full((3 * D,), ratio[0]), jnp.full((D,), ratio[1]), jnp.full((TD,), ratio[2])])
    attn_new = attn_w - learn_rate * ratio_cols[None, :] * attn_update
    mlp_new = mlp_w - learn_rate * ratio[3:5][:, None, None] * mlp_update
    norm_ratio = jnp.sqrt(jnp.sum(norm_w * norm_w)) / jnp.sqrt(jnp.sum(norm_update * norm_update))
    norm_new = norm_w - learn_rate * norm_ratio * norm_update
    return (block_out.astype(jnp.bfloat16), grad_x, attn_new, attn_first_new, attn_second_new, mlp_new, mlp_first_new, mlp_second_new, norm_new, norm_first_new, norm_second_new, lamb_norms)
```

```python
import functools
import jax
import jax.numpy as jnp
from jax import lax
from jax.experimental import pallas as pl
from jax.experimental.pallas import tpu as pltpu
from jax.sharding import PartitionSpec as P

D = 768
H = 12
HD = 64
FF = 3072
TD = 1024
T = 1024
LONGEST = 312
STEP = 10
QB = 128
TB = 256
FB = 768
GB = 512
F32 = jnp.float32
BF16 = jnp.bfloat16

eps_norm = 1e-06
beta_one = 0.9
beta_two = 0.999
eps_adam = 1e-06
decay_rate = 0.05
learn_rate = 0.3


def dot(a, b):
    return jnp.dot(a, b, preferred_element_type=F32)


def dot_t(a, b):
    return lax.dot_general(a, b, (((1,), (1,)), ((), ())), preferred_element_type=F32)


def norm_parts(values):
    centre = values - jnp.mean(values, axis=-1, keepdims=True)
    inv = lax.rsqrt(jnp.mean(centre * centre, axis=-1, keepdims=True) + eps_norm)
    return centre * inv, inv


def norm_back(grad, normed, inv, gain):
    scaled = grad * gain
    first = jnp.mean(scaled, axis=-1, keepdims=True)
    second = jnp.mean(scaled * normed, axis=-1, keepdims=True)
    return (scaled - first - normed * second) * inv


def window(block):
    low = max(0, (block * QB - (LONGEST - 1)) // QB * QB)
    high = min(T, -(-(block * QB + QB + LONGEST - 1) // QB) * QB)
    return low, high


def rows(index, size):
    return pl.ds(pl.multiple_of(index * size, size), size)


def compute_kernel(x_ref, seg_ref, gain_ref, shift_ref, tgt_hbm, cot_hbm, wa_hbm, wm_hbm,
                   y_hbm, xg_ref, ga_hbm, gm_hbm, small_ref,
                   wa, wm, gq, proj, h1t, ctxt, h2t, h3t, got, hid, gpre, tg, cot, ctx,
                   kaug, qaug, kt, vt, gka, gva, lse, delta, sem):
    loads = []
    for i, (src, dst) in enumerate(((wa_hbm, wa), (wm_hbm, wm), (tgt_hbm, tg), (cot_hbm, cot))):
        copy = pltpu.make_async_copy(src, dst, sem.at[i])
        copy.start()
        loads.append(copy)

    small_ref[...] = jnp.zeros_like(small_ref)
    marks = lax.broadcasted_iota(jnp.int32, (128, T), 0)
    same = jnp.where(marks == seg_ref[...], 1.0, 0.0).T
    kaug[:, 128:] = same.astype(BF16)
    lane = lax.broadcasted_iota(jnp.int32, (T, 128), 1)
    apart = jnp.where((lane < 8) & (same == 0.0), -1e30, 0.0).astype(BF16)
    for b in range(T // QB):
        for half in range(2):
            qaug[b * 2 * QB + half * QB:b * 2 * QB + (half + 1) * QB, 128:] = apart[b * QB:(b + 1) * QB]

    loads[0].wait()

    def first(i, _):
        r = rows(i, TB)
        hat, _inv = norm_parts(x_ref[r, :].astype(F32))
        h1 = (hat * gain_ref[0:1, :] + shift_ref[0:1, :]).astype(BF16)
        h1t[:, r] = h1.T
        proj[r, :] = dot(h1, wa[:, :3 * D]).astype(BF16)
        return 0

    lax.fori_loop(0, T // TB, first, 0)

    low_lane = lax.broadcasted_iota(jnp.int32, (QB, 128), 1) < HD
    low_row = lax.broadcasted_iota(jnp.int32, (128, QB), 0) < HD

    def slab(p, part):
        return pl.ds(pl.multiple_of(part * D + p * 128, 128), 128)

    def stage_pair(p):
        kaug[:, :128] = proj[:, slab(p, 1)]
        for b in range(T // QB):
            q = proj[b * QB:(b + 1) * QB, slab(p, 0)] * jnp.asarray(HD ** -0.5, BF16)
            qaug[b * 2 * QB:b * 2 * QB + QB, :128] = jnp.where(low_lane, q, jnp.zeros_like(q))
            qaug[b * 2 * QB + QB:(b + 1) * 2 * QB, :128] = jnp.where(low_lane, jnp.zeros_like(q), q)

    def attend(p, _):
        stage_pair(p)
        vt[...] = proj[:, slab(p, 2)].T
        for b in range(T // QB):
            low, high = window(b)
            s = dot_t(kaug[low:high, :], qaug[b * 2 * QB:(b + 1) * 2 * QB, :])
            top = jnp.max(s, axis=0, keepdims=True)
            e = jnp.exp(s - top)
            total = jnp.sum(e, axis=0, keepdims=True)
            r = dot(vt[:, low:high], e.astype(BF16)) / total
            c = jnp.where(low_row, r[:, :QB], r[:, QB:])
            lse[p, b:b + 1, :] = top + jnp.log(total)
            ctxt[pl.ds(pl.multiple_of(p * 128, 128), 128), b * QB:(b + 1) * QB] = c.astype(BF16)
            ctx[b * QB:(b + 1) * QB, slab(p, 0)] = c.T.astype(BF16)
        return 0

    lax.fori_loop(0, H // 2, attend, 0)
    loads[1].wait()

    def up(i, _):
        r = rows(i, TB)
        mid = x_ref[r, :].astype(F32) + dot(ctx[r, :], wa[:, 3 * D:4 * D])
        xg_ref[r, :] = mid
        hat, _inv = norm_parts(mid)
        h2 = (hat * gain_ref[1:2, :] + shift_ref[1:2, :]).astype(BF16)
        h2t[:, r] = h2.T

        for j in range(FF // FB):
            c = slice(j * FB, (j + 1) * FB)
            pre = dot(h2, wm[0, :, c])
            cdf = 0.5 * (1.0 + lax.erf(pre * 0.7071067811865476))
            pdf = jnp.exp(-0.5 * pre * pre) * 0.3989422804014327
            hid[r, c] = (pre * cdf).astype(BF16)
            gpre[r, c] = (cdf + pre * pdf).astype(BF16)
        return 0

    lax.fori_loop(0, T // TB, up, 0)
    loads[2].wait()
    loads[3].wait()
    head_of = (lax.broadcasted_iota(jnp.int32, (16, D), 1) // HD
               == lax.broadcasted_iota(jnp.int32, (16, D), 0)).astype(BF16)

    def down(i, _):
        r = rows(i, TB)
        mid = xg_ref[r, :]
        out = mid + dot_t(hid[r, :], wm[1])
        hat, inv = norm_parts(out)
        h3 = (hat * gain_ref[2:3, :] + shift_ref[2:3, :]).astype(BF16)
        h3t[:, r] = h3.T
        al = dot(h3, wa[:, 4 * D:])
        t = tg[r, :].astype(F32)
        ra = lax.rsqrt(jnp.mean(al * al, axis=-1, keepdims=True) + eps_norm)
        rt = lax.rsqrt(jnp.mean(t * t, axis=-1, keepdims=True) + eps_norm)
        c = jnp.mean(al * t, axis=-1, keepdims=True)
        gal = (-(ra * rt) * (t - c * ra * ra * al)).astype(BF16)
        tg[r, :] = gal
        g3 = dot_t(gal, wa[:, 4 * D:])
        small_ref[2:3, :] += jnp.sum(g3 * hat, axis=0, keepdims=True)
        small_ref[5:6, :] += jnp.sum(g3, axis=0, keepdims=True)
        gout = cot[r, :].astype(F32) + norm_back(g3, hat, inv, gain_ref[2:3, :])
        cot[r, :] = out.astype(BF16)
        low = gout.astype(BF16)
        got[:, r] = low.T
        for j in range(FF // FB):
            c = slice(j * FB, (j + 1) * FB)
            gpre[r, c] = (dot(low, wm[1, :, c]) * gpre[r, c].astype(F32)).astype(BF16)
        g2 = dot_t(gpre[r, :], wm[0])
        hat2, inv2 = norm_parts(mid)
        small_ref[1:2, :] += jnp.sum(g2 * hat2, axis=0, keepdims=True)
        small_ref[4:5, :] += jnp.sum(g2, axis=0, keepdims=True)
        gmid = gout + norm_back(g2, hat2, inv2, gain_ref[1:2, :])
        xg_ref[r, :] = gmid
        gc = dot_t(gmid.astype(BF16), wa[:, 3 * D:4 * D]).astype(BF16)
        e = ctx[r, :].astype(F32) * gc.astype(F32)
        e_high = e.astype(BF16)
        sums = dot_t(head_of, e_high) + dot_t(head_of, (e - e_high.astype(F32)).astype(BF16))
        for h in range(H):
            delta[h, :, r] = sums[h:h + 1, :]
        ctx[r, :] = gc
        return 0

    lax.fori_loop(0, T // TB, down, 0)
    y_copy = pltpu.make_async_copy(cot, y_hbm, sem.at[0])
    y_copy.start()

    wa[:, 4 * D:] = dot(h3t[...], tg[...]).astype(BF16)

    def ffgrad(j, _):
        c = rows(j, GB)
        wm[1, :, c] = dot(got[...], hid[:, c]).astype(BF16)
        wm[0, :, c] = dot(h2t[...], gpre[:, c]).astype(BF16)
        return 0

    lax.fori_loop(0, FF // GB, ffgrad, 0)
    wa[:, 3 * D:4 * D] = dot(ctxt[...], xg_ref[...].astype(BF16)).astype(BF16)

    def attend_back(p, _):
        stage_pair(p)
        kt[...] = proj[:, slab(p, 1)].T
        for b in range(T // QB):
            low, high = window(b)
            qs = slice(b * QB, (b + 1) * QB)
            q = qaug[b * 2 * QB:(b + 1) * 2 * QB, :]
            g = ctx[qs, slab(p, 0)]
            zero = jnp.zeros_like(g)
            g2 = jnp.concatenate([jnp.where(low_lane, g, zero), jnp.where(low_lane, zero, g)], axis=0)
            s = dot_t(kaug[low:high, :], q)
            prob = jnp.exp(s - lse[p, b:b + 1, :])
            dp = dot_t(proj[low:high, slab(p, 2)], g2)
            off = jnp.concatenate([delta[2 * p, :, qs], delta[2 * p + 1, :, qs]], axis=1)
            ds = (prob * (dp - off)).astype(BF16)
            pb = prob.astype(BF16)
            gk = dot(ds, q[:, :128])
            gv = dot(pb, g2)
            new = (0 if b == 0 else window(b - 1)[1])
            for lo, hi, fresh in ((low, min(new, high), False), (max(low, new), high, True)):
                if lo < hi:
                    a, z = lo - low, hi - low
                    gka[lo:hi, :] = gk[a:z] if fresh else gka[lo:hi, :] + gk[a:z]
                    gva[lo:hi, :] = gv[a:z] if fresh else gva[lo:hi, :] + gv[a:z]
            r = dot(kt[:, low:high], ds)
            c = jnp.where(low_row, r[:, :QB], r[:, QB:]) * HD ** -0.5
            proj[qs, slab(p, 0)] = c.T.astype(BF16)
        proj[:, slab(p, 1)] = gka[...].astype(BF16)
        proj[:, slab(p, 2)] = gva[...].astype(BF16)
        return 0

    lax.fori_loop(0, H // 2, attend_back, 0)

    for j in range(3):
        gq[:, j * D:(j + 1) * D] = dot(h1t[...], proj[:, j * D:(j + 1) * D]).astype(BF16)

    def last(i, _):
        r = rows(i, TB)
        g1 = dot_t(proj[r, :], wa[:, :3 * D])
        hat, inv = norm_parts(x_ref[r, :].astype(F32))
        small_ref[0:1, :] += jnp.sum(g1 * hat, axis=0, keepdims=True)
        small_ref[3:4, :] += jnp.sum(g1, axis=0, keepdims=True)
        xg_ref[r, :] += norm_back(g1, hat, inv, gain_ref[0:1, :])
        return 0

    lax.fori_loop(0, T // TB, last, 0)
    y_copy.wait()
    stores = []
    for i, (src, dst) in enumerate(((gq, ga_hbm.at[:, :3 * D]), (wa.at[:, 3 * D:], ga_hbm.at[:, 3 * D:]), (wm, gm_hbm))):
        copy = pltpu.make_async_copy(src, dst, sem.at[i])
        copy.start()
        stores.append(copy)
    for copy in stores:
        copy.wait()


def compute(x, seg, gain, shift, tgt, cot, wa, wm):
    vmem = pl.BlockSpec(memory_space=pltpu.VMEM)
    hbm = pl.BlockSpec(memory_space=pl.ANY)
    sds = jax.ShapeDtypeStruct
    return pl.pallas_call(
        compute_kernel,
        out_shape=(sds((T, D), BF16), sds((T, D), F32), sds((D, 4 * D + TD), BF16), sds((2, D, FF), BF16), sds((8, D), F32)),
        in_specs=[vmem, vmem, vmem, vmem, hbm, hbm, hbm, hbm],
        out_specs=(hbm, vmem, hbm, hbm, vmem),
        scratch_shapes=[
            pltpu.VMEM((D, 4 * D + TD), BF16), pltpu.VMEM((2, D, FF), BF16), pltpu.VMEM((D, 3 * D), BF16),
            pltpu.VMEM((T, 3 * D), BF16), pltpu.VMEM((D, T), BF16), pltpu.VMEM((D, T), BF16),
            pltpu.VMEM((D, T), BF16), pltpu.VMEM((D, T), BF16), pltpu.VMEM((D, T), BF16),
            pltpu.VMEM((T, FF), BF16), pltpu.VMEM((T, FF), BF16), pltpu.VMEM((T, TD), BF16),
            pltpu.VMEM((T, D), BF16), pltpu.VMEM((T, D), BF16),
            pltpu.VMEM((T, 256), BF16), pltpu.VMEM((2 * T, 256), BF16), pltpu.VMEM((128, T), BF16), pltpu.VMEM((128, T), BF16),
            pltpu.VMEM((T, 128), F32), pltpu.VMEM((T, 128), F32), pltpu.VMEM((H // 2, T // QB, 2 * QB), F32),
            pltpu.VMEM((H, 1, T), F32), pltpu.SemaphoreType.DMA((4,)),
        ],
        compiler_params=pltpu.CompilerParams(vmem_limit_bytes=67043328),
        name="block_step",
    )(x, seg, gain, shift, tgt, cot, wa, wm)


def moments(weight, gradient, first_old, second_old, wd_rate):
    first_new = beta_one * first_old + (1.0 - beta_one) * gradient
    second_new = beta_two * second_old + (1.0 - beta_two) * gradient * gradient
    corr_one = 1.0 - beta_one**STEP
    corr_two = 1.0 - beta_two**STEP
    update = first_new / corr_one / (jnp.sqrt(second_new / corr_two) + eps_adam) + wd_rate * weight
    return (first_new, second_new, update)


def on_device(
    x_in,
    segments,
    targets,
    cotangent,
    norm_gain,
    norm_bias,
    attn_w,
    mlp_w,
    norm_first,
    norm_second,
    attn_first,
    attn_second,
    mlp_first,
    mlp_second,
):
    w_attn = lax.all_gather(attn_w.astype(BF16), ("dp", "mp"), axis=0, tiled=True)
    w_mlp = lax.all_gather(mlp_w.astype(BF16), "dp", axis=1, tiled=True)
    w_mlp = lax.all_gather(w_mlp, "mp", axis=2, tiled=True)
    y_out, grad_in, part_attn, part_mlp, part_small = compute(
        x_in, segments, norm_gain, norm_bias, targets, cotangent, w_attn, w_mlp
    )
    grad_mlp = lax.psum_scatter(part_mlp, "dp", scatter_dimension=1, tiled=True)
    grad_mlp = lax.psum_scatter(grad_mlp, "mp", scatter_dimension=2, tiled=True).astype(F32)
    grad_attn = lax.psum_scatter(part_attn, ("dp", "mp"), scatter_dimension=0, tiled=True).astype(F32)
    small_grad = lax.psum(part_small[:6], ("dp", "mp"))
    attn_first_new, attn_second_new, attn_update = moments(
        attn_w, grad_attn, attn_first, attn_second, decay_rate
    )
    mlp_first_new, mlp_second_new, mlp_update = moments(
        mlp_w, grad_mlp, mlp_first, mlp_second, decay_rate
    )
    col_weight = jnp.sum(attn_w * attn_w, axis=0)
    col_update = jnp.sum(attn_update * attn_update, axis=0)
    weight_sq = jnp.stack(
        [
            jnp.sum(col_weight[: 3 * D]),
            jnp.sum(col_weight[3 * D : 4 * D]),
            jnp.sum(col_weight[4 * D :]),
            jnp.sum(mlp_w[0] * mlp_w[0]),
            jnp.sum(mlp_w[1] * mlp_w[1]),
        ]
    )
    update_sq = jnp.stack(
        [
            jnp.sum(col_update[: 3 * D]),
            jnp.sum(col_update[3 * D : 4 * D]),
            jnp.sum(col_update[4 * D :]),
            jnp.sum(mlp_update[0] * mlp_update[0]),
            jnp.sum(mlp_update[1] * mlp_update[1]),
        ]
    )
    local_stats = jnp.stack([weight_sq, update_sq])
    totals = lax.psum(local_stats, ("dp", "mp"))
    lamb_norms = jnp.sqrt(totals)
    ratio = lamb_norms[0] / lamb_norms[1]
    ratio_cols = jnp.concatenate(
        [jnp.full((3 * D,), ratio[0]), jnp.full((D,), ratio[1]), jnp.full((TD,), ratio[2])]
    )
    attn_new = attn_w - learn_rate * ratio_cols[None, :] * attn_update
    mlp_new = mlp_w - learn_rate * ratio[3:5][:, None, None] * mlp_update
    norm_w = jnp.concatenate([norm_gain, norm_bias], axis=0)
    norm_first_new, norm_second_new, norm_update = moments(
        norm_w, small_grad, norm_first, norm_second, 0.0
    )
    norm_ratio = jnp.sqrt(jnp.sum(norm_w * norm_w)) / jnp.sqrt(jnp.sum(norm_update * norm_update))
    norm_new = norm_w - learn_rate * norm_ratio * norm_update
    return (
        y_out,
        grad_in,
        attn_new,
        attn_first_new,
        attn_second_new,
        mlp_new,
        mlp_first_new,
        mlp_second_new,
        norm_new,
        norm_first_new,
        norm_second_new,
        lamb_norms,
    )


def solution(mesh):
    placed = (
        P(("dp", "mp"), None),
        P(("dp", "mp"), None),
        P(("dp", "mp"), None),
        P(("dp", "mp"), None),
        P(),
        P(),
        P(("dp", "mp"), None),
        P(None, "dp", "mp"),
        P(),
        P(),
        P(("dp", "mp"), None),
        P(("dp", "mp"), None),
        P(None, "dp", "mp"),
        P(None, "dp", "mp"),
    )
    return jax.shard_map(
        on_device,
        mesh=mesh,
        in_specs=placed,
        out_specs=(
            P(("dp", "mp"), None),
            P(("dp", "mp"), None),
            P(("dp", "mp"), None),
            P(("dp", "mp"), None),
            P(("dp", "mp"), None),
            P(None, "dp", "mp"),
            P(None, "dp", "mp"),
            P(None, "dp", "mp"),
            P(),
            P(),
            P(),
            P(),
        ),
        check_vma=False,
    )
```

```python
import functools
import jax
import jax.numpy as jnp
from jax import lax
from jax.experimental import pallas as pl
from jax.experimental.pallas import tpu as pltpu
from jax.sharding import PartitionSpec as P

D = 768
H = 12
HD = 64
FF = 3072
TD = 1024
T = 1024
LONGEST = 312
STEP = 10
QB = 128
TB = 256
FB = 768
GB = 512
F32 = jnp.float32
BF16 = jnp.bfloat16

eps_norm = 1e-06
beta_one = 0.9
beta_two = 0.999
eps_adam = 1e-06
decay_rate = 0.05
learn_rate = 0.3


def dot(a, b):
    return jnp.dot(a, b, preferred_element_type=F32)


def dot_t(a, b):
    return lax.dot_general(a, b, (((1,), (1,)), ((), ())), preferred_element_type=F32)


def norm_parts(values):
    centre = values - jnp.mean(values, axis=-1, keepdims=True)
    inv = lax.rsqrt(jnp.mean(centre * centre, axis=-1, keepdims=True) + eps_norm)
    return centre * inv, inv


def norm_back(grad, normed, inv, gain):
    scaled = grad * gain
    first = jnp.mean(scaled, axis=-1, keepdims=True)
    second = jnp.mean(scaled * normed, axis=-1, keepdims=True)
    return (scaled - first - normed * second) * inv


def window(block):
    low = max(0, (block * QB - (LONGEST - 1)) // QB * QB)
    high = min(T, -(-(block * QB + QB + LONGEST - 1) // QB) * QB)
    return low, high


def rows(index, size):
    return pl.ds(pl.multiple_of(index * size, size), size)


FIVE = (2, 2, 2, 2, 2)
Z2, Z1, X, Y, C = range(5)
ALL = slice(None)


class Place:
    def __init__(self):
        dp, mp = lax.axis_index("dp"), lax.axis_index("mp")
        self.mine = (lax.rem(lax.div(dp, 4), 2), lax.rem(lax.div(dp, 2), 2), lax.rem(dp, 2), lax.div(mp, 2), lax.rem(mp, 2))
        self.dp, self.mp = dp, mp

    def partner(self, bit):
        turn = 1 - 2 * self.mine[bit]
        if bit <= X:
            return {"dp": self.dp + turn * (4, 2, 1)[bit], "mp": self.mp}
        return {"dp": self.dp, "mp": self.mp + turn * (2, 1)[bit - Y]}


class Piece:
    def __init__(self, ref, lead, row, col):
        self.ref, self.lead, self.row, self.col = ref, lead, row, col

    def where(self, bits):
        return (*self.lead, *bits, self.row, self.col)

    def at(self, bits):
        return self.ref.at[self.where(bits)]


class Gather:
    def __init__(self, place, piece, order, send, recv):
        self.copies, self.step, self.live = [], -1, True
        for j, bit in enumerate(order):
            view = piece.at(tuple(ALL if d in order[:j] else place.mine[d] for d in range(5)))
            self.copies.append(pltpu.make_async_remote_copy(
                view, view, send.at[j], recv.at[j], device_id=place.partner(bit), device_id_type=pl.DeviceIdType.MESH))

    def go(self):
        if self.step >= 0:
            self.copies[self.step].wait()
        self.step += 1
        if self.step < 5:
            self.copies[self.step].start()

    def finish(self):
        while self.step < 5:
            self.go()


class Scatter:
    def __init__(self, place, piece, order, lands, send, recv, out):
        self.copies, self.step, self.out = [], -1, out
        self.place, self.piece, self.order, self.lands = place, piece, order, lands
        for j, bit in enumerate(order):
            view = piece.at(tuple(1 - place.mine[d] if d == bit else place.mine[d] if d in order[:j] else ALL for d in range(5)))
            land = lands[j].at((ALL,) * (4 - j))
            self.copies.append(pltpu.make_async_remote_copy(
                view, land, send.at[j], recv.at[j], device_id=place.partner(bit), device_id_type=pl.DeviceIdType.MESH))

    def go(self):
        if self.step >= 0:
            j = self.step
            self.copies[j].wait()
            left = [d for d in range(5) if d not in self.order[:j + 1]]
            piece, land, mine = self.piece, self.lands[j], self.place.mine

            def add(i, _):
                at = [lax.rem(lax.div(i, 2 ** (len(left) - 1 - k)), 2) for k in range(len(left))]
                bits = tuple(at[left.index(d)] if d in left else mine[d] for d in range(5))
                here, there = piece.where(bits), land.where(tuple(at))
                if j == 4:
                    self.out(piece.ref[here].astype(F32) + land.ref[there].astype(F32))
                else:
                    piece.ref[here] = piece.ref[here] + land.ref[there]
                return 0

            if left:
                lax.fori_loop(0, 2 ** len(left), add, 0)
            else:
                add(0, 0)
        self.step += 1
        if self.step < 5:
            self.copies[self.step].start()

    def finish(self):
        while self.step < 5:
            self.go()


class Total:
    def __init__(self, place, ref, land, send, recv):
        self.ref, self.land, self.step = ref, land, -1
        self.copies = [pltpu.make_async_remote_copy(
            ref, land.at[j], send.at[j], recv.at[j], device_id=place.partner(j), device_id_type=pl.DeviceIdType.MESH) for j in range(5)]

    def go(self):
        if self.step >= 0:
            self.copies[self.step].wait()
            self.ref[...] = self.ref[...] + self.land[self.step]
        self.step += 1
        if self.step < 5:
            self.copies[self.step].start()


def step_kernel(comm, *refs):
    (x_ref, seg_ref, gain_ref, shift_ref, tgt_hbm, cot_hbm, wa_in, wm_in,
     y_hbm, xg_ref, ga_out, gm_out, small_ref, *refs) = refs
    (wa, wm, gq, proj, h1t, ctxt, h2t, h3t, got, hid, gpre, tg, cot, ctx,
     kaug, qaug, kt, gka, gva, lse, delta, sem, *refs) = refs
    everywhere = (ALL,) * 5

    def wide(cols):
        return wa[(*everywhere, ALL, cols)].reshape(D, -1)

    def tall(m, j):
        return wm[(m, ALL, ALL, ALL, j // 2, j % 2)].reshape(D, FB)

    loads = [pltpu.make_async_copy(src, dst, sem.at[i]) for i, (src, dst) in enumerate(((tgt_hbm, tg), (cot_hbm, cot)))]
    if not comm:
        loads += [pltpu.make_async_copy(src, dst, sem.at[i + 2]) for i, (src, dst) in enumerate(((wa_in, wa), (wm_in, wm)))]
    for copy in loads:
        copy.start()
    small_ref[...] = jnp.zeros_like(small_ref)

    qkv_cols, out_cols, head_cols = slice(0, 3 * D), slice(3 * D, 4 * D), slice(4 * D, 4 * D + TD)
    half_a, half_b = slice(0, 9 * 128), slice(9 * 128, 3 * D)
    if comm:
        ag_send, ag_recv, rs_send, rs_recv, ready, sm_send, sm_recv, sm_land = refs
        place = Place()
        mine = place.mine
        wa[(*mine, ALL, ALL)] = wa_in[...].astype(BF16)
        for m in range(2):
            wm[(m, *mine, ALL, ALL)] = wm_in[m].astype(BF16)
        barrier = pltpu.get_barrier_semaphore()
        for bit in range(5):
            pl.semaphore_signal(barrier, inc=1, device_id=place.partner(bit), device_id_type=pl.DeviceIdType.MESH)
        pl.semaphore_wait(barrier, 5)
        xy, yx = (Z2, Z1, X, Y, C), (Z2, Z1, Y, X, C)

        def gather(k, piece, order):
            return Gather(place, piece, order, ag_send.at[k], ag_recv.at[k])

        ag_a = gather(0, Piece(wa, (), ALL, half_a), xy)
        ag_b = gather(1, Piece(wa, (), ALL, half_b), yx)
        ag_out = gather(2, Piece(wa, (), ALL, out_cols), xy)
        ag_up = gather(3, Piece(wm, (0,), ALL, ALL), xy)
        ag_down = gather(4, Piece(wm, (1,), ALL, ALL), yx)
        ag_head = gather(5, Piece(wa, (), ALL, head_cols), yx)
        rest = (ag_up, ag_down, ag_out, ag_head)
        ag_a.go()
        ag_b.go()

    marks = lax.broadcasted_iota(jnp.int32, (128, T), 0)
    same = jnp.where(marks == seg_ref[...], 1.0, 0.0).T
    kaug[:, 128:] = same.astype(BF16)
    lane = lax.broadcasted_iota(jnp.int32, (T, 128), 1)
    apart = jnp.where((lane < 8) & (same == 0.0), -1e30, 0.0).astype(BF16)
    for b in range(T // QB):
        for half in range(2):
            qaug[b * 2 * QB + half * QB:b * 2 * QB + (half + 1) * QB, 128:] = apart[b * QB:(b + 1) * QB]

    def enter(i, _):
        r = rows(i, TB)
        hat, _inv = norm_parts(x_ref[r, :].astype(F32))
        h1 = (hat * gain_ref[0:1, :] + shift_ref[0:1, :]).astype(BF16)
        h1t[:, r] = h1.T
        ctx[r, :] = h1
        return 0

    lax.fori_loop(0, T // TB, enter, 0)
    if comm:
        ag_a.go()
        ag_b.go()
        for g in rest:
            g.go()
        ag_a.go()
        ag_b.go()
        for g in rest:
            g.go()
        ag_a.go()
        ag_b.go()
        ag_a.go()
        ag_b.go()
        for g in rest:
            g.go()
        ag_a.go()
        ag_b.go()
    else:
        for copy in loads[2:]:
            copy.wait()

    def first(i, _):
        r = rows(i, TB)
        proj[r, :] = dot(ctx[r, :], wide(qkv_cols)).astype(BF16)
        return 0

    lax.fori_loop(0, T // TB, first, 0)

    low_lane = lax.broadcasted_iota(jnp.int32, (QB, 128), 1) < HD
    low_row = lax.broadcasted_iota(jnp.int32, (128, QB), 0) < HD

    def slab(p, part):
        return pl.ds(pl.multiple_of(part * D + p * 128, 128), 128)

    def stage_pair(p):
        kaug[:, :128] = proj[:, slab(p, 1)]
        for b in range(T // QB):
            q = proj[b * QB:(b + 1) * QB, slab(p, 0)] * jnp.asarray(HD ** -0.5, BF16)
            qaug[b * 2 * QB:b * 2 * QB + QB, :128] = jnp.where(low_lane, q, jnp.zeros_like(q))
            qaug[b * 2 * QB + QB:(b + 1) * 2 * QB, :128] = jnp.where(low_lane, jnp.zeros_like(q), q)

    def ticks(p, plan):
        for at, chains in plan.items():
            @pl.when(p == at)
            def _():
                for chain in chains:
                    chain.go()

    plan = {1: (ag_up, ag_out), 2: (ag_down, ag_head), 4: (ag_up, ag_out), 5: (ag_down, ag_head)} if comm else {}

    def attend(p, _):
        stage_pair(p)
        kt[...] = proj[:, slab(p, 2)].T
        for b in range(T // QB):
            low, high = window(b)
            s = dot_t(kaug[low:high, :], qaug[b * 2 * QB:(b + 1) * 2 * QB, :])
            top = jnp.max(s, axis=0, keepdims=True)
            e = jnp.exp(s - top)
            total = jnp.sum(e, axis=0, keepdims=True)
            r = dot(kt[:, low:high], e.astype(BF16)) / total
            c = jnp.where(low_row, r[:, :QB], r[:, QB:])
            lse[p, b:b + 1, :] = top + jnp.log(total)
            ctxt[pl.ds(pl.multiple_of(p * 128, 128), 128), b * QB:(b + 1) * QB] = c.astype(BF16)
            ctx[b * QB:(b + 1) * QB, slab(p, 0)] = c.T.astype(BF16)
        ticks(p, plan)
        return 0

    lax.fori_loop(0, H // 2, attend, 0)
    if comm:
        ag_up.finish()
        ag_out.finish()

    def block_of(ref, j, i):
        return (j // 2, j % 2, lax.div(i, 2), lax.rem(i, 2))

    def up(i, _):
        r = rows(i, TB)
        mid = x_ref[r, :].astype(F32) + dot(ctx[r, :], wide(out_cols))
        xg_ref[r, :] = mid
        hat, _inv = norm_parts(mid)
        h2 = (hat * gain_ref[1:2, :] + shift_ref[1:2, :]).astype(BF16)
        h2t[(*everywhere, ALL, r)] = h2.T.reshape(*FIVE, 24, TB)
        for j in range(FF // FB):
            pre = dot(h2, tall(0, j))
            cdf = 0.5 * (1.0 + lax.erf(pre * 0.7071067811865476))
            pdf = jnp.exp(-0.5 * pre * pre) * 0.3989422804014327
            hid[block_of(hid, j, i)] = (pre * cdf).astype(BF16).reshape(2, 128, FB)
            gpre[block_of(gpre, j, i)] = (cdf + pre * pdf).astype(BF16).reshape(2, 128, FB)
        return 0

    lax.fori_loop(0, T // TB, up, 0)
    loads[0].wait()
    loads[1].wait()
    if comm:
        ag_down.finish()
        ag_head.finish()
    head_of = (lax.broadcasted_iota(jnp.int32, (16, D), 1) // HD
               == lax.broadcasted_iota(jnp.int32, (16, D), 0)).astype(BF16)

    def down(i, _):
        r = rows(i, TB)
        mid = xg_ref[r, :]
        out = mid
        for j in range(FF // FB):
            out = out + dot_t(hid[block_of(hid, j, i)].reshape(TB, FB), tall(1, j))
        hat, inv = norm_parts(out)
        h3 = (hat * gain_ref[2:3, :] + shift_ref[2:3, :]).astype(BF16)
        h3t[(*everywhere, ALL, r)] = h3.T.reshape(*FIVE, 24, TB)
        al = dot(h3, wide(head_cols))
        blk = (lax.div(i, 2), lax.rem(i, 2))
        t = tg[blk].reshape(TB, TD).astype(F32)
        ra = lax.rsqrt(jnp.mean(al * al, axis=-1, keepdims=True) + eps_norm)
        rt = lax.rsqrt(jnp.mean(t * t, axis=-1, keepdims=True) + eps_norm)
        c = jnp.mean(al * t, axis=-1, keepdims=True)
        gal = (-(ra * rt) * (t - c * ra * ra * al)).astype(BF16)
        tg[blk] = gal.reshape(2, 2, 2, 32, TD)
        g3 = dot_t(gal, wide(head_cols))
        small_ref[2:3, :] += jnp.sum(g3 * hat, axis=0, keepdims=True)
        small_ref[5:6, :] += jnp.sum(g3, axis=0, keepdims=True)
        gout = cot[r, :].astype(F32) + norm_back(g3, hat, inv, gain_ref[2:3, :])
        cot[r, :] = out.astype(BF16)
        low = gout.astype(BF16)
        got[(*everywhere, ALL, r)] = low.T.reshape(*FIVE, 24, TB)
        g2 = jnp.zeros((TB, D), F32)
        for j in range(FF // FB):
            at = block_of(gpre, j, i)
            gp = (dot(low, tall(1, j)) * gpre[at].reshape(TB, FB).astype(F32)).astype(BF16)
            gpre[at] = gp.reshape(2, 128, FB)
            g2 = g2 + dot_t(gp, tall(0, j))
        hat2, inv2 = norm_parts(mid)
        small_ref[1:2, :] += jnp.sum(g2 * hat2, axis=0, keepdims=True)
        small_ref[4:5, :] += jnp.sum(g2, axis=0, keepdims=True)
        gmid = gout + norm_back(g2, hat2, inv2, gain_ref[1:2, :])
        xg_ref[r, :] = gmid
        gc = dot_t(gmid.astype(BF16), wide(out_cols)).astype(BF16)
        e = ctx[r, :].astype(F32) * gc.astype(F32)
        e_high = e.astype(BF16)
        sums = dot_t(head_of, e_high) + dot_t(head_of, (e - e_high.astype(F32)).astype(BF16))
        for h in range(H):
            delta[h, :, r] = sums[h:h + 1, :]
        ctx[r, :] = gc
        return 0

    lax.fori_loop(0, T // TB, down, 0)
    y_copy = pltpu.make_async_copy(cot, y_hbm, sem.at[0])
    y_copy.start()

    if comm:
        xyz, yxz = (C, X, Y, Z1, Z2), (C, Y, X, Z1, Z2)
        leads = ((0,), (1, 0), (1, 1, 0), (1, 1, 1, 0), (1, 1, 1, 1, 0))

        def inside(ref, row, col):
            return [Piece(ref, lead, row, col) for lead in leads]

        def scatter(k, piece, order, lands, out):
            return Scatter(place, piece, order, lands, rs_send.at[k], rs_recv.at[k], out)

        def into(ref, at):
            def put(value):
                ref[at] = value
            return put

        low96, low24 = slice(0, 96), slice(96, 120)
        rs_down = scatter(0, Piece(wm, (1,), ALL, ALL), xyz, inside(hid, low96, ALL), into(gm_out, 1))
        rs_up = scatter(1, Piece(wm, (0,), ALL, ALL), yxz, inside(gpre, low96, ALL), into(gm_out, 0))
        rs_head = scatter(2, Piece(wa, (), ALL, head_cols), yxz, inside(h3t, ALL, ALL),
                          into(ga_out, (ALL, head_cols)))
        rs_out = scatter(3, Piece(wa, (), ALL, out_cols), xyz, inside(hid, low24, ALL), into(ga_out, (ALL, out_cols)))
        rs_qkv = []
        for k in range(3):
            cols = slice(k * D, (k + 1) * D)
            rs_qkv.append(scatter(4 + k, Piece(gq, (), ALL, cols), xyz if k % 2 else yxz,
                                  inside((h2t, got, tg)[k], slice(0, 24), slice(0, D)), into(ga_out, (ALL, cols))))

        def meet(k):
            for bit in range(5):
                pl.semaphore_signal(ready.at[k], inc=1, device_id=place.partner(bit), device_id_type=pl.DeviceIdType.MESH)
            pl.semaphore_wait(ready.at[k], 5)

    def fold(ref, m, lhs):
        def part(j, _):
            a, b = lax.div(j, 2), lax.rem(j, 2)
            g = dot(lhs[...].reshape(D, T), ref[a, b].reshape(T, FB)).astype(BF16)
            wm[m, :, :, :, a, b] = g.reshape(2, 2, 2, 96, FB)
            return 0

        lax.fori_loop(0, FF // FB, part, 0)

    wa[(*everywhere, ALL, head_cols)] = dot(h3t[...].reshape(D, T), tg[...].reshape(T, TD)).astype(BF16).reshape(*FIVE, 24, TD)
    fold(hid, 1, got)
    if comm:
        meet(0)
        rs_down.go()
        rs_head.go()
    wa[(*everywhere, ALL, out_cols)] = dot(ctxt[...], xg_ref[...].astype(BF16)).astype(BF16).reshape(*FIVE, 24, D)
    if comm:
        rs_out.go()
        rs_down.go()
    fold(gpre, 0, h2t)
    if comm:
        meet(1)
        rs_up.go()
        rs_head.go()
        plan = {0: (rs_up, rs_out), 1: (rs_down, rs_head), 2: (rs_up, rs_out), 3: (rs_down, rs_head), 4: (rs_up, rs_out), 5: (rs_down, rs_head)}

    def attend_back(p, _):
        stage_pair(p)
        kt[...] = proj[:, slab(p, 1)].T
        for b in range(T // QB):
            low, high = window(b)
            qs = slice(b * QB, (b + 1) * QB)
            q = qaug[b * 2 * QB:(b + 1) * 2 * QB, :]
            g = ctx[qs, slab(p, 0)]
            zero = jnp.zeros_like(g)
            g2 = jnp.concatenate([jnp.where(low_lane, g, zero), jnp.where(low_lane, zero, g)], axis=0)
            s = dot_t(kaug[low:high, :], q)
            prob = jnp.exp(s - lse[p, b:b + 1, :])
            dp = dot_t(proj[low:high, slab(p, 2)], g2)
            off = jnp.concatenate([delta[2 * p, :, qs], delta[2 * p + 1, :, qs]], axis=1)
            ds = (prob * (dp - off)).astype(BF16)
            pb = prob.astype(BF16)
            gk = dot(ds, q[:, :128])
            gv = dot(pb, g2)
            new = (0 if b == 0 else window(b - 1)[1])
            for lo, hi, fresh in ((low, min(new, high), False), (max(low, new), high, True)):
                if lo < hi:
                    a, z = lo - low, hi - low
                    gka[lo:hi, :] = gk[a:z] if fresh else gka[lo:hi, :] + gk[a:z]
                    gva[lo:hi, :] = gv[a:z] if fresh else gva[lo:hi, :] + gv[a:z]
            r = dot(kt[:, low:high], ds)
            c = jnp.where(low_row, r[:, :QB], r[:, QB:]) * HD ** -0.5
            proj[qs, slab(p, 0)] = c.T.astype(BF16)
        proj[:, slab(p, 1)] = gka[...].astype(BF16)
        proj[:, slab(p, 2)] = gva[...].astype(BF16)
        ticks(p, plan)
        return 0

    lax.fori_loop(0, H // 2, attend_back, 0)

    for k in range(3):
        cols = slice(k * D, (k + 1) * D)
        gq[(*everywhere, ALL, cols)] = dot(h1t[...], proj[:, cols]).astype(BF16).reshape(*FIVE, 24, D)
        if comm:
            rs_qkv[k].go()
    if comm:
        rs_up.go()
        rs_out.go()

    def last(i, _):
        r = rows(i, TB)
        g1 = dot_t(proj[r, :], wide(qkv_cols))
        hat, inv = norm_parts(x_ref[r, :].astype(F32))
        small_ref[0:1, :] += jnp.sum(g1 * hat, axis=0, keepdims=True)
        small_ref[3:4, :] += jnp.sum(g1, axis=0, keepdims=True)
        xg_ref[r, :] += norm_back(g1, hat, inv, gain_ref[0:1, :])
        return 0

    lax.fori_loop(0, T // TB, last, 0)
    y_copy.wait()
    if comm:
        total = Total(place, small_ref, sm_land, sm_send, sm_recv)
        for k in range(6):
            total.go()
            for chain in (*rs_qkv, rs_down, rs_head, rs_up, rs_out):
                if chain.step < 5:
                    chain.go()
    else:
        stores = [pltpu.make_async_copy(src, dst, sem.at[i]) for i, (src, dst) in enumerate((
            (gq, ga_out.at[(*everywhere, ALL, qkv_cols)]),
            (wa.at[(*everywhere, ALL, slice(3 * D, 4 * D + TD))], ga_out.at[(*everywhere, ALL, slice(3 * D, 4 * D + TD))]),
            (wm, gm_out)))]
        for copy in stores:
            copy.start()
        for copy in stores:
            copy.wait()


def compute(comm, x, seg, gain, shift, tgt, cot, wa, wm):
    vmem = pl.BlockSpec(memory_space=pltpu.VMEM)
    hbm = pl.BlockSpec(memory_space=pl.ANY)
    sds = jax.ShapeDtypeStruct
    dma = pltpu.SemaphoreType.DMA
    cols = 4 * D + TD
    scratch = [
        pltpu.VMEM((*FIVE, 24, cols), BF16), pltpu.VMEM((2, *FIVE, 96, FB), BF16), pltpu.VMEM((*FIVE, 24, 3 * D), BF16),
        pltpu.VMEM((T, 3 * D), BF16), pltpu.VMEM((D, T), BF16), pltpu.VMEM((D, T), BF16),
        pltpu.VMEM((*FIVE, 24, T), BF16), pltpu.VMEM((*FIVE, 24, T), BF16), pltpu.VMEM((*FIVE, 24, T), BF16),
        pltpu.VMEM((*FIVE, 128, FB), BF16), pltpu.VMEM((*FIVE, 128, FB), BF16), pltpu.VMEM((*FIVE, 32, TD), BF16),
        pltpu.VMEM((T, D), BF16), pltpu.VMEM((T, D), BF16),
        pltpu.VMEM((T, 256), BF16), pltpu.VMEM((2 * T, 256), BF16), pltpu.VMEM((128, T), BF16),
        pltpu.VMEM((T, 128), F32), pltpu.VMEM((T, 128), F32), pltpu.VMEM((H // 2, T // QB, 2 * QB), F32),
        pltpu.VMEM((H, 1, T), F32), dma((4,)),
    ]
    if comm:
        scratch += [dma((6, 5)), dma((6, 5)), dma((7, 5)), dma((7, 5)), pltpu.SemaphoreType.REGULAR((2,)), dma((5,)), dma((5,)),
                    pltpu.VMEM((5, 8, D), F32)]
        out_w = (sds((24, cols), F32), sds((2, 96, FB), F32))
        params = pltpu.CompilerParams(vmem_limit_bytes=67043328, collective_id=0, has_side_effects=True)
    else:
        out_w = (sds((*FIVE, 24, cols), BF16), sds((2, *FIVE, 96, FB), BF16))
        params = pltpu.CompilerParams(vmem_limit_bytes=67043328)
    w = vmem if comm else hbm
    return pl.pallas_call(
        functools.partial(step_kernel, comm),
        out_shape=(sds((T, D), BF16), sds((T, D), F32), *out_w, sds((8, D), F32)),
        in_specs=[vmem, vmem, vmem, vmem, hbm, hbm, w, w],
        out_specs=(hbm, vmem, w, w, vmem),
        scratch_shapes=scratch,
        compiler_params=params,
        name="block_step",
    )(x, seg, gain, shift, tgt.reshape(*FIVE, 32, TD), cot, wa, wm)


def stats_kernel(n_dp, n_mp, in_ref, out_ref, land, send, recv):
    dp, mp = lax.axis_index("dp"), lax.axis_index("mp")
    partners, size = [], 1
    while size < n_mp:
        partners.append({"dp": dp, "mp": mp + size * (1 - 2 * lax.rem(lax.div(mp, size), 2))})
        size *= 2
    size = 1
    while size < n_dp:
        partners.append({"dp": dp + size * (1 - 2 * lax.rem(lax.div(dp, size), 2)), "mp": mp})
        size *= 2
    barrier = pltpu.get_barrier_semaphore()
    for other in partners:
        pl.semaphore_signal(barrier, inc=1, device_id=other, device_id_type=pl.DeviceIdType.MESH)
    out_ref[...] = in_ref[...]
    pl.semaphore_wait(barrier, len(partners))
    for j, other in enumerate(partners):
        copy = pltpu.make_async_remote_copy(out_ref, land.at[j], send.at[j], recv.at[j], device_id=other, device_id_type=pl.DeviceIdType.MESH)
        copy.start()
        copy.wait()
        out_ref[...] = out_ref[...] + land[j]


def all_sum(value, n_dp, n_mp):
    bits = (n_dp * n_mp).bit_length() - 1
    vmem = pl.BlockSpec(memory_space=pltpu.VMEM)
    return pl.pallas_call(
        functools.partial(stats_kernel, n_dp, n_mp),
        out_shape=jax.ShapeDtypeStruct(value.shape, F32),
        in_specs=[vmem],
        out_specs=vmem,
        scratch_shapes=[pltpu.VMEM((bits, *value.shape), F32), pltpu.SemaphoreType.DMA((bits,)), pltpu.SemaphoreType.DMA((bits,))],
        compiler_params=pltpu.CompilerParams(collective_id=1, has_side_effects=True),
        name="stats_sum",
    )(value)


def moments(weight, gradient, first_old, second_old, wd_rate):
    first_new = beta_one * first_old + (1.0 - beta_one) * gradient
    second_new = beta_two * second_old + (1.0 - beta_two) * gradient * gradient
    corr_one = 1.0 - beta_one**STEP
    corr_two = 1.0 - beta_two**STEP
    update = first_new / corr_one / (jnp.sqrt(second_new / corr_two) + eps_adam) + wd_rate * weight
    return (first_new, second_new, update)


def on_device(
    n_dp,
    n_mp,
    x_in,
    segments,
    targets,
    cotangent,
    norm_gain,
    norm_bias,
    attn_w,
    mlp_w,
    norm_first,
    norm_second,
    attn_first,
    attn_second,
    mlp_first,
    mlp_second,
):
    if n_dp == 8 and n_mp == 4:
        y_out, grad_in, grad_attn, grad_mlp, small_grad = compute(
            True, x_in, segments, norm_gain, norm_bias, targets, cotangent, attn_w, mlp_w
        )
        small_grad = small_grad[:6]
    else:
        w_attn = lax.all_gather(attn_w.astype(BF16), ("dp", "mp"), axis=0, tiled=True)
        w_mlp = lax.all_gather(mlp_w.astype(BF16), "dp", axis=1, tiled=True)
        w_mlp = lax.all_gather(w_mlp, "mp", axis=2, tiled=True)
        y_out, grad_in, part_attn, part_mlp, part_small = compute(
            False, x_in, segments, norm_gain, norm_bias, targets, cotangent, w_attn.reshape(*FIVE, 24, -1),
            w_mlp.reshape(2, 8, 96, 4, FB).transpose(0, 1, 3, 2, 4).reshape(2, *FIVE, 96, FB)
        )
        part_mlp = part_mlp.reshape(2, 8, 4, 96, FB).transpose(0, 1, 3, 2, 4).reshape(2, D, FF)
        grad_mlp = lax.psum_scatter(part_mlp, "dp", scatter_dimension=1, tiled=True)
        grad_mlp = lax.psum_scatter(grad_mlp, "mp", scatter_dimension=2, tiled=True).astype(F32)
        grad_attn = lax.psum_scatter(part_attn.reshape(D, -1), ("dp", "mp"), scatter_dimension=0, tiled=True).astype(F32)
        small_grad = lax.psum(part_small[:6], ("dp", "mp"))
    attn_first_new, attn_second_new, attn_update = moments(
        attn_w, grad_attn, attn_first, attn_second, decay_rate
    )
    mlp_first_new, mlp_second_new, mlp_update = moments(
        mlp_w, grad_mlp, mlp_first, mlp_second, decay_rate
    )
    col_weight = jnp.sum(attn_w * attn_w, axis=0)
    col_update = jnp.sum(attn_update * attn_update, axis=0)
    weight_sq = jnp.stack(
        [
            jnp.sum(col_weight[: 3 * D]),
            jnp.sum(col_weight[3 * D : 4 * D]),
            jnp.sum(col_weight[4 * D :]),
            jnp.sum(mlp_w[0] * mlp_w[0]),
            jnp.sum(mlp_w[1] * mlp_w[1]),
        ]
    )
    update_sq = jnp.stack(
        [
            jnp.sum(col_update[: 3 * D]),
            jnp.sum(col_update[3 * D : 4 * D]),
            jnp.sum(col_update[4 * D :]),
            jnp.sum(mlp_update[0] * mlp_update[0]),
            jnp.sum(mlp_update[1] * mlp_update[1]),
        ]
    )
    local_stats = jnp.stack([weight_sq, update_sq])
    totals = all_sum(jnp.pad(local_stats, ((0, 6), (0, 123))), n_dp, n_mp)[:2, :5]
    lamb_norms = jnp.sqrt(totals)
    ratio = lamb_norms[0] / lamb_norms[1]
    ratio_cols = jnp.concatenate(
        [jnp.full((3 * D,), ratio[0]), jnp.full((D,), ratio[1]), jnp.full((TD,), ratio[2])]
    )
    attn_new = attn_w - learn_rate * ratio_cols[None, :] * attn_update
    mlp_new = mlp_w - learn_rate * ratio[3:5][:, None, None] * mlp_update
    norm_w = jnp.concatenate([norm_gain, norm_bias], axis=0)
    norm_first_new, norm_second_new, norm_update = moments(
        norm_w, small_grad, norm_first, norm_second, 0.0
    )
    norm_ratio = jnp.sqrt(jnp.sum(norm_w * norm_w)) / jnp.sqrt(jnp.sum(norm_update * norm_update))
    norm_new = norm_w - learn_rate * norm_ratio * norm_update
    return (
        y_out,
        grad_in,
        attn_new,
        attn_first_new,
        attn_second_new,
        mlp_new,
        mlp_first_new,
        mlp_second_new,
        norm_new,
        norm_first_new,
        norm_second_new,
        lamb_norms,
    )


def solution(mesh):
    placed = (
        P(("dp", "mp"), None),
        P(("dp", "mp"), None),
        P(("dp", "mp"), None),
        P(("dp", "mp"), None),
        P(),
        P(),
        P(("dp", "mp"), None),
        P(None, "dp", "mp"),
        P(),
        P(),
        P(("dp", "mp"), None),
        P(("dp", "mp"), None),
        P(None, "dp", "mp"),
        P(None, "dp", "mp"),
    )
    return jax.shard_map(
        functools.partial(on_device, mesh.shape["dp"], mesh.shape["mp"]),
        mesh=mesh,
        in_specs=placed,
        out_specs=(
            P(("dp", "mp"), None),
            P(("dp", "mp"), None),
            P(("dp", "mp"), None),
            P(("dp", "mp"), None),
            P(("dp", "mp"), None),
            P(None, "dp", "mp"),
            P(None, "dp", "mp"),
            P(None, "dp", "mp"),
            P(),
            P(),
            P(),
            P(),
        ),
        check_vma=False,
    )
```
